32 devices in a mesh: blk: 8 (over z, y), rep: 4 (over x, core).
Axes of the slice: x: 2, y: 2, z: 4, core: 2. Of those that a mesh axis runs over, the one named last changes fastest.
Arguments:
- embeddings: bfloat16 [3072, 1024], P(('blk', 'rep')), may hold values from -60 to 60, as said below
Outputs:
- nearest: float32 [3072, 8], P(('blk', 'rep'))
- dup_count: float32 [3072], P(('blk', 'rep'))
The draws below stay inside these ranges and needn't reach their ends.
Inputs may be any that keep to these rules, and one draw needn't show every extreme that they name: Real-valued embeddings; no row is zero.
All inputs are finite; a program needn't handle non-finite values.
Results may differ from the reference program's by a relative error of at most 0.00068.
Values may be sent and summed in bfloat16 or wider, within the bound.
A program may use at most 128 MiB of HBM per device.

```python
import math
import jax
import jax.numpy as jnp
from jax import lax

D = 1024
TOPK = 8
NROWS = 3072
NCLUST = 384
N_BLK = 8


def draw_embeddings(key, part):
    keys = jax.random.split(key, 5)
    labels = jax.random.randint(keys[0], (NROWS,), 0, NCLUST)
    centers = jax.random.normal(keys[1], (NCLUST, D), jnp.float32)
    noise = jax.random.normal(keys[2], (NROWS, D), jnp.float32)
    blend_factor = jax.random.uniform(keys[3], (NROWS, 1), jnp.float32, 0.3, 0.95)
    scales = jnp.exp(jax.random.uniform(keys[4], (NROWS, 1), jnp.float32, 0.0, math.log(10.0)))
    rows = blend_factor * centers[labels] + jnp.sqrt(1.0 - blend_factor * blend_factor) * noise
    return jnp.clip(rows * scales, -60.0, 60.0).astype(jnp.bfloat16)


def setup_inputs(seed: int = 0) -> dict:
    seeds = jax.random.split(jax.random.key(seed), 2)
    embeddings = draw_embeddings(jax.random.fold_in(seeds[1], 71), 0)
    return {"embeddings": embeddings}


decision_bound = 0.5
sigmoid_sharpness = 0.05

def reference(embeddings):
    whole = embeddings.astype(jnp.float32)
    unit = (whole / jnp.sqrt(lax.optimization_barrier(jnp.sum(whole * whole, axis=1, keepdims=True)) + 1e-06)).astype(jnp.bfloat16)
    block_rows = NROWS // N_BLK
    all_ids = jnp.arange(NROWS, dtype=jnp.int32)

    def single_tile(index):
        queries = lax.dynamic_slice_in_dim(unit, index * block_rows, block_rows, 0)
        query_ids = index * block_rows + jnp.arange(block_rows, dtype=jnp.int32)
        cosine_table = jnp.dot(queries, unit.T, preferred_element_type=jnp.float32)
        cosine_table = jnp.where(query_ids[:, None] == all_ids[None, :], -2.0, cosine_table)
        best = lax.top_k(cosine_table, TOPK)[0]
        duplicate_tally = lax.optimization_barrier(jnp.sum(jax.nn.sigmoid((cosine_table - decision_bound) / sigmoid_sharpness), axis=1))
        return (best, duplicate_tally)
    best, duplicate_tally = lax.map(single_tile, jnp.arange(N_BLK, dtype=jnp.int32))
    return (best.reshape(NROWS, TOPK), duplicate_tally.reshape(NROWS))
```

```python
import math

import jax
import jax.numpy as jnp
from jax import lax
from jax.experimental import pallas as pl
from jax.experimental.pallas import tpu as pltpu
from jax.sharding import PartitionSpec as P

TOPK = 8
SUB, LANES = 8, 128


decision_bound = 0.5
sigmoid_sharpness = 0.05


def joined(shard, axis, combine):
    everything = jax.tree.map(lambda part: lax.all_gather(part, axis), shard)
    initial = jax.tree.map(lambda part: part[0], everything)

    def lap(k, so_far):
        return combine(so_far, jax.tree.map(lambda part: part[k], everything))

    return lax.fori_loop(1, lax.axis_size(axis), lap, initial)


def unit_rows(block):
    whole = block.astype(jnp.float32)
    return (whole / jnp.sqrt(jnp.sum(whole * whole, axis=1, keepdims=True) + 1e-06)).astype(
        jnp.bfloat16
    )


def top_values(table):
    columns = lax.broadcasted_iota(jnp.int32, table.shape, 1)
    picked = []
    for rank in range(TOPK):
        largest = jnp.max(table, axis=1)
        first_hit = jnp.min(jnp.where(table == largest[:, None], columns, table.shape[1]), axis=1)
        table = jnp.where(columns == first_hit[:, None], -jnp.inf, table)
        picked.append(largest)
    return jnp.stack(picked, axis=1)


def score(queries, query_ids, keys, key_ids, carry):
    cosine_table = lax.dot_general(
        queries, keys, (((1,), (1,)), ((), ())), preferred_element_type=jnp.float32
    )
    cosine_table = jnp.where(query_ids[:, None] == key_ids[None, :], -2.0, cosine_table)
    best = top_values(jnp.concatenate([carry[0], cosine_table], axis=1))
    duplicate_tally = jnp.sum(
        jax.nn.sigmoid((cosine_table - decision_bound) / sigmoid_sharpness), axis=1
    )
    return (best, duplicate_tally)


def join_lists(first, runner_value):
    best = top_values(jnp.concatenate([first[0], runner_value[0]], axis=1))
    return (best, first[1] + runner_value[1])


def body(embeddings):
    rows = embeddings.shape[0]
    reps = lax.axis_size("rep")
    copy_number = lax.axis_index("rep")
    tile_number = lax.axis_index("blk")
    unit = unit_rows(embeddings)
    queries = lax.all_gather(unit, "rep", axis=0, tiled=True)
    query_ids = tile_number * reps * rows + jnp.arange(reps * rows, dtype=jnp.int32)
    start_lists = (
        jnp.full((reps * rows, TOPK), -2.0, jnp.float32),
        jnp.zeros((reps * rows,), jnp.float32),
    )
    piece = lax.all_gather(unit, "blk", axis=0, tiled=True)
    position = jnp.arange(piece.shape[0], dtype=jnp.int32)
    key_ids = (position // rows * reps + copy_number) * rows + position % rows
    lists = score(queries, query_ids, piece, key_ids, start_lists)
    best, duplicate_tally = joined(lists, "rep", join_lists)
    offset = copy_number * rows
    nearest = lax.dynamic_slice_in_dim(best, offset, rows, 0)
    dup_count = lax.dynamic_slice_in_dim(duplicate_tally, offset, rows, 0)
    return (nearest, dup_count)


PLAN = {"blk": 8, "rep": 4}
PLANE = 4
CHUNKS = 3
MESH = pl.DeviceIdType.MESH

SORT8 = (
    (0, 1), (2, 3), (4, 5), (6, 7),
    (0, 2), (1, 3), (4, 6), (5, 7),
    (1, 2), (5, 6),
    (0, 4), (1, 5), (2, 6), (3, 7),
    (2, 4), (3, 5),
    (1, 2), (3, 4), (5, 6),
)


def exchange(items, pairs):
    items = list(items)
    for i, j in pairs:
        items[i], items[j] = jnp.maximum(items[i], items[j]), jnp.minimum(items[i], items[j])
    return items


def in_order(items):
    if len(items) == TOPK:
        return exchange(items, SORT8)
    pairs = [(j, j + 1) for end in range(len(items) - 1, 0, -1) for j in range(end)]
    return exchange(items, pairs)


def merged(best, other):
    size = len(other)
    best = [
        jnp.maximum(best[i], other[TOPK - 1 - i]) if TOPK - 1 - i < size else best[i]
        for i in range(TOPK)
    ]
    pairs = [
        (i, i + step) for step in (4, 2, 1) for i in range(TOPK) if i // step % 2 == 0
    ]
    return exchange(best, pairs)


def duplicates(sim):
    scale = -math.log2(math.e) / sigmoid_sharpness
    return 1.0 / (1.0 + jnp.exp2((sim - decision_bound) * scale))


def take_in(sim_ref, keys, lanes, state, fresh):
    width = min(lanes, LANES)

    def tile(t, _):
        start = 0 if lanes <= LANES else pl.multiple_of(t * LANES, LANES)
        part = pl.ds(start, width)
        best = None if fresh else [state[k, :, part] for k in range(TOPK)]
        count = jnp.zeros((SUB, width), jnp.float32) if fresh else state[TOPK, :, part]
        for group in range(0, keys, SUB * TOPK):
            rows = [
                sim_ref[pl.ds(row, SUB), part]
                for row in range(group, min(group + SUB * TOPK, keys), SUB)
            ]
            for row in rows:
                count = count + duplicates(row)
            rows = in_order(rows)
            best = rows if best is None else merged(best, rows)
        for k in range(TOPK):
            state[k, :, part] = best[k]
        state[TOPK, :, part] = count
        return 0

    if lanes <= LANES:
        tile(0, 0)
    else:
        lax.fori_loop(0, lanes // LANES, tile, 0)


def across_rows(best, count):
    for step in (4, 2, 1):
        best = merged(best, [pltpu.roll(item, step, axis=0) for item in best])
        if count is not None:
            count = count + pltpu.roll(count, step, axis=0)
    row = lax.broadcasted_iota(jnp.int32, best[0].shape, 0)
    joined_list = best[0]
    for k in range(1, TOPK):
        joined_list = jnp.where(row == k, best[k], joined_list)
    return joined_list, count


def against(keys, queries):
    return lax.dot_general(keys, queries, (((1,), (1,)), ((), ())), preferred_element_type=jnp.float32)


def direct_kernel(
    x_ref, near_ref, dup_ref, raw, plane, far, sim_own, sim_pair, sim_cross, sim_last,
    own_state, plane_state, cross_state, whole, result, arrived,
    raw_sem, send, recv, fwd_send, fwd_recv, res_send, res_recv,
):
    rows, width = x_ref.shape
    step = rows // CHUNKS
    blk, rep = lax.axis_index("blk"), lax.axis_index("rep")
    y, z, core, x = blk % 2, blk // 2, rep % 2, rep // 2
    inner = (z == 1) | (z == 2)

    def place(px, py, pz, other_core=0):
        return (pz * 2 + py, px * 2 + (core + other_core) % 2)

    partner = place(x, y, z, 1)
    along_x, along_y = place(1 - x, y, z), place(x, 1 - y, z)
    pair = place(x, y, z + 1 - 2 * (z % 2))
    middle = place(x, y, 3 - z)
    source = place(x, y, (1 - z // 2) * (3 - z) + z // 2 * (z - 2))
    relay_to = place(x, y, (2 - z) * 2)

    barrier = pltpu.get_barrier_semaphore()

    def greet(device):
        pl.semaphore_signal(barrier, inc=1, device_id=device, device_id_type=MESH)

    for peer in (partner, along_x, along_y, pair):
        greet(peer)

    @pl.when(inner)
    def _():
        greet(middle)

    fetch = pltpu.make_async_copy(x_ref, raw, raw_sem)
    fetch.start()
    fetch.wait()
    plane[0, 0] = unit_rows(raw[...])

    pl.semaphore_wait(barrier, 4 + z * (3 - z) // 2)

    def part(c):
        return pl.ds(c * step, step)

    def move(src, dst, send_to, recv_from, c, device):
        return pltpu.make_async_remote_copy(
            src_ref=src.at[part(c)], dst_ref=dst.at[part(c)],
            send_sem=send.at[send_to, c], recv_sem=recv.at[recv_from, c],
            device_id=device, device_id_type=MESH,
        )

    own = plane.at[0, 0]
    order = range(CHUNKS)
    backward = range(CHUNKS - 1, -1, -1)

    def to_middle(c):
        return move(own, far.at[3 - z], 3, 3 + 3 - z, c, middle)

    def relay_pair(c):
        return move(far.at[0], far.at[1], 4, 4, c, relay_to)

    def relay_transit(c):
        return move(far.at[2], far.at[1], 5, 4, c, pair)

    to_x = [move(own, plane.at[1, 0], 0, 0, c, along_x) for c in order]
    to_y = [move(own, plane.at[2, 0], 1, 1, c, along_y) for c in order]
    to_pair = [move(own, far.at[0], 2, 3, c, pair) for c in order]
    arrives = [move(far.at[0], far.at[1], 4, 4, c, pair) for c in order]
    relay_xy = [
        move(plane.at[2, 0], plane.at[3, 0], 6, 2, c, along_x)
        if c == CHUNKS - 1
        else move(plane.at[1, 0], plane.at[3, 0], 6, 2, c, along_y)
        for c in order
    ]

    @pl.when(inner)
    def _():
        for c in order:
            to_middle(c).start()

    for c, d in zip(order, backward):
        to_pair[c].start()
        to_x[c].start()
        to_y[d].start()
    forwards = [
        pltpu.make_async_remote_copy(
            src_ref=plane.at[slot, 0], dst_ref=plane.at[slot, 1],
            send_sem=fwd_send.at[slot], recv_sem=fwd_recv.at[slot],
            device_id=partner, device_id_type=MESH,
        )
        for slot in range(PLANE)
    ]
    forwards[0].start()

    def relay_far(c):
        @pl.when(z == 2)
        def _():
            move(far.at[2], far.at[2], 5, 5, c, pair).wait_recv()
            relay_transit(c).start()

        to_pair[c].wait_recv()

        @pl.when(inner)
        def _():
            relay_pair(c).start()

    query = plane[0, 0]
    sim = against(query, query)
    key_id = lax.broadcasted_iota(jnp.int32, sim.shape, 0)
    query_id = lax.broadcasted_iota(jnp.int32, sim.shape, 1)
    sim_own[0:rows] = jnp.where(key_id == query_id, -2.0, sim)
    forwards[0].wait_recv()
    sim_own[rows:] = against(plane[0, 1], query)
    take_in(sim_own, 2 * rows, rows, own_state, True)

    for c, d in zip(order, backward):
        to_x[c].wait_recv()
        if c < CHUNKS - 1:
            relay_xy[c].start()
        to_y[d].wait_recv()
        if d == CHUNKS - 1:
            relay_xy[d].start()
        relay_far(c)
    forwards[1].start()
    forwards[2].start()

    for slot in (1, 2):
        forwards[slot].wait_recv()
        sim_own[...] = against(plane[slot].reshape(2 * rows, width), query)
        take_in(sim_own, 2 * rows, rows, own_state, False)
    for copy in relay_xy:
        copy.wait_recv()
    forwards[3].start()
    forwards[3].wait_recv()
    sim_own[...] = against(plane[3].reshape(2 * rows, width), query)
    take_in(sim_own, 2 * rows, rows, own_state, False)

    lanes = 2 * PLANE * rows

    def plane_rows():
        return plane[...].reshape(lanes, width)

    sim_pair[...] = against(far[0], plane_rows())
    take_in(sim_pair, rows, lanes, plane_state, True)

    for c in range(CHUNKS - 1):
        arrives[c].wait_recv()
    head = rows - step
    if head:
        sim_pair[0:head] = against(far[1, 0:head], plane_rows())
        take_in(sim_pair, head, lanes, plane_state, False)
    arrives[-1].wait_recv()
    sim_cross[...] = against(plane_rows(), far[1])
    take_in(sim_cross, lanes, rows, cross_state, True)

    def give(slot, device):
        gift = pltpu.make_async_remote_copy(
            src_ref=result.at[slot], dst_ref=arrived.at[slot],
            send_sem=res_send.at[slot], recv_sem=res_recv.at[slot],
            device_id=device, device_id_type=MESH,
        )
        gift.start()
        return gift

    last = 2 * PLANE
    best, count = across_rows([cross_state[k] for k in range(TOPK)], cross_state[TOPK])
    result[last, 0, :, 0:rows] = best
    result[last, 1, :, 0:rows] = count
    gifts = [give(last, source)]

    sim_last[...] = against(far[1, head:rows], plane_rows())
    take_in(sim_last, step, lanes, plane_state, False)
    for start in range(0, lanes, LANES):
        tile = slice(start, start + LANES)
        best, count = across_rows([plane_state[k, :, tile] for k in range(TOPK)], plane_state[TOPK, :, tile])
        whole[0, :, tile] = best
        whole[1, :, tile] = count
    for slot in (6, 7, 2, 3, 4, 5, 1):
        result[slot, :, :, 0:rows] = whole[:, :, slot * rows : (slot + 1) * rows]
        chip = (x, y), (1 - x, y), (x, 1 - y), (1 - x, 1 - y)
        gifts.append(give(slot, place(*chip[slot // 2], z, slot % 2)))

    best, count = across_rows([own_state[k] for k in range(TOPK)], own_state[TOPK])
    lists = [best, whole[0, :, 0:rows]]
    count = count + whole[1, :, 0:rows]
    for gift, slot in zip(gifts, (last, 6, 7, 2, 3, 4, 5, 1)):
        gift.wait_recv()
        lists.append(arrived[slot, 0, :, 0:rows])
        count = count + arrived[slot, 1, :, 0:rows]
    best = merged(in_order(lists[:TOPK]), in_order(lists[TOPK:]))
    near_ref[...], _ = across_rows(best, None)
    dup_ref[...] = count[0]

    for copy in [*to_x, *to_y, *to_pair, *relay_xy, *forwards, *gifts]:
        copy.wait_send()

    @pl.when(inner)
    def _():
        for c in order:
            to_middle(c).wait_send()
            relay_pair(c).wait_send()

    @pl.when(z == 2)
    def _():
        for c in order:
            relay_transit(c).wait_send()


def hand_out(near_ref, dup_ref, near_out, dup_out, sems):
    copies = [
        pltpu.make_async_copy(src, dst, sems.at[i])
        for i, (src, dst) in enumerate(((near_ref, near_out), (dup_ref, dup_out)))
    ]
    for copy in copies:
        copy.start()
    for copy in copies:
        copy.wait()


def direct_body(embeddings):
    rows, width = embeddings.shape
    f32 = jnp.float32
    wide = -(-rows // LANES) * LANES
    lanes = 2 * PLANE * rows
    dma = pltpu.SemaphoreType.DMA
    out = pl.pallas_call(
        direct_kernel,
        out_shape=(pltpu.VMEM((SUB, rows), f32), pltpu.VMEM((rows,), f32)),
        in_specs=[pl.BlockSpec(memory_space=pl.ANY)],
        out_specs=(pl.BlockSpec(memory_space=pltpu.VMEM),) * 2,
        scratch_shapes=[
            pltpu.VMEM((rows, width), embeddings.dtype),
            pltpu.VMEM((PLANE, 2, rows, width), jnp.bfloat16),
            pltpu.VMEM((3, rows, width), jnp.bfloat16),
            pltpu.VMEM((2 * rows, rows), f32),
            pltpu.VMEM((rows, lanes), f32),
            pltpu.VMEM((lanes, rows), f32),
            pltpu.VMEM((rows // CHUNKS, lanes), f32),
            pltpu.VMEM((TOPK + 1, SUB, rows), f32),
            pltpu.VMEM((TOPK + 1, SUB, lanes), f32),
            pltpu.VMEM((TOPK + 1, SUB, rows), f32),
            pltpu.VMEM((2, SUB, lanes), f32),
            pltpu.VMEM((2 * PLANE + 1, 2, SUB, wide), f32),
            pltpu.VMEM((2 * PLANE + 1, 2, SUB, wide), f32),
            dma,
            dma((7, CHUNKS)),
            dma((6, CHUNKS)),
            dma((PLANE,)),
            dma((PLANE,)),
            dma((2 * PLANE + 1,)),
            dma((2 * PLANE + 1,)),
        ],
        compiler_params=pltpu.CompilerParams(collective_id=0, has_side_effects=True),
    )(embeddings)
    near, dup = pl.pallas_call(
        hand_out,
        out_shape=(jax.ShapeDtypeStruct((SUB, rows), f32), jax.ShapeDtypeStruct((rows,), f32)),
        in_specs=[pl.BlockSpec(memory_space=pltpu.VMEM)] * 2,
        out_specs=(pl.BlockSpec(memory_space=pl.ANY),) * 2,
        scratch_shapes=[dma((2,))],
    )(*(pltpu.with_memory_space_constraint(part, pltpu.VMEM) for part in out))
    return near.T, dup


def solution(mesh):
    placed = (P(("blk", "rep"), None),)
    direct = all(mesh.shape[axis] == size for axis, size in PLAN.items())
    return jax.shard_map(
        direct_body if direct else body,
        mesh=mesh,
        in_specs=placed,
        out_specs=(P(("blk", "rep"), None), P(("blk", "rep"))),
        check_vma=False,
    )
```
